32 devices in a mesh: gz: 2 (over z_hi), gy: 4 (over z_lo, core), gx: 4 (over y, x).
Axes of the slice: x: 2, y: 2, z: 4 (z_hi: 2, z_lo: 2; z = z_hi * 2 + z_lo), core: 2. Of those that a mesh axis runs over, the one named last changes fastest.
Arguments:
- charges: float32 [65536], P(('gz', 'gy', 'gx')), may hold values from -2.5 to 2.5
- fractions: float32 [3, 65536], P(None, ('gz', 'gy', 'gx')), may hold values from 0 to 1
- base_cells: int32 [3, 65536], P(None, ('gz', 'gy', 'gx')), may hold values from 0 to 255, as said below
- counts: int32 [2, 4, 4], P('gz', 'gy', 'gx'), may hold values from 1024 to 2048, as said below
Outputs:
- forces: float32 [3, 65536], P(None, ('gz', 'gy', 'gx'))
The draws below stay inside these ranges and needn't reach their ends.
Inputs may be any that keep to these rules, and one draw needn't show every extreme that they name: `base_cells`: atom slots of the block at gz, gy, gx have base cells inside that block's cells: x in gx*64 to gx*64 + 63, y in gy*64 to gy*64 + 63, z in gz*128 to gz*128 + 127. The first counts[b] slots of block b hold atoms, the rest are empty; some block is full in every draw.
All inputs are finite; a program needn't handle non-finite values.
Results may differ from the reference program's by a relative error of at most 0.0003.
Values sent between devices are 32-bit elements; how exact they have to be, the bound alone decides.
A program may use at most 256 MiB of HBM per device.

```python
import jax
import jax.numpy as jnp

GRID = 256
ORDER = 4
CAP = 2048
CX = 64
CY = 64
CZ = 128
ATOMS = 65536


def draw_base_cells(key, part):
    blocks_x = GRID // CX
    blocks_y = GRID // CY
    blocks_z = GRID // CZ
    slot_index = jnp.arange(CAP * blocks_x * blocks_y * blocks_z, dtype=jnp.int32)
    block = slot_index // CAP
    block_x = block % blocks_x
    block_y = block // blocks_x % blocks_y
    block_z = block // (blocks_x * blocks_y)
    base_key = jax.random.fold_in(key, 11)
    key_x = jax.random.fold_in(base_key, 1)
    key_y = jax.random.fold_in(base_key, 2)
    key_z = jax.random.fold_in(base_key, 3)
    cell_x = block_x * CX + jax.random.randint(key_x, slot_index.shape, 0, CX, dtype=jnp.int32)
    cell_y = block_y * CY + jax.random.randint(key_y, slot_index.shape, 0, CY, dtype=jnp.int32)
    cell_z = block_z * CZ + jax.random.randint(key_z, slot_index.shape, 0, CZ, dtype=jnp.int32)
    return jnp.stack([cell_x, cell_y, cell_z]).astype(jnp.int32)


def draw_counts(key, part):
    blocks_x = GRID // CX
    blocks_y = GRID // CY
    blocks_z = GRID // CZ
    total = blocks_x * blocks_y * blocks_z
    base_key = jax.random.fold_in(key, 23)
    values = jax.random.randint(jax.random.fold_in(base_key, 1), (total,), CAP // 2, CAP + 1, dtype=jnp.int32)
    chosen = jax.random.randint(jax.random.fold_in(base_key, 2), (), 0, total, dtype=jnp.int32)
    values = jnp.where(jnp.arange(total, dtype=jnp.int32) == chosen, CAP, values)
    return values.reshape(blocks_z, blocks_y, blocks_x).astype(jnp.int32)


def block_levels(rng, dims, pieces, smallest, high):
    loudness, own = 1.0, jax.random.fold_in(rng, 6)
    for dim, blocks in pieces:
        heights = jnp.exp(jax.random.uniform(jax.random.fold_in(own, dim), (blocks,), jnp.float32, smallest / len(pieces), high / len(pieces)))
        loudness = loudness * jnp.repeat(heights, dims[dim] // blocks).reshape([-1 if axis == dim else 1 for axis in range(len(dims))])
    return loudness


def gaussian(key, shape, deviation, bound, split=(), held_as=jnp.bfloat16):
    loudness = block_levels(key, shape, split, -0.22, 0.18) if split else 1.0
    values = jax.random.normal(key, shape, jnp.float32) * deviation * loudness
    return jnp.minimum(jnp.maximum(values, -bound), bound).astype(held_as)


def setup_inputs(seed: int = 0) -> dict:
    splits = jax.random.split(jax.random.key(seed), 5)
    return {
        "charges": gaussian(splits[0], (ATOMS,), 0.4, 2.5, ((0, 32),), jnp.float32),
        "fractions": jnp.clip(1.0 * jax.random.uniform(splits[1], (3, ATOMS), jnp.float32) ** block_levels(splits[1], (3, ATOMS), ((1, 32),), -0.2, 0.2), 0.0, 1.0),
        "base_cells": draw_base_cells(jax.random.fold_in(splits[4], 71), 0),
        "counts": draw_counts(jax.random.fold_in(splits[4], 71), 0),
    }


coulomb = 332.0636
ewald = 0.7


def spline_weights(frac):
    rest = 1.0 - frac
    square = frac * frac
    cube = square * frac
    weights = jnp.stack([rest * rest * rest / 6.0, (3.0 * cube - 6.0 * square + 4.0) / 6.0,
                         (-3.0 * cube + 3.0 * square + 3.0 * frac + 1.0) / 6.0, cube / 6.0])
    slopes = jnp.stack([-0.5 * rest * rest, 1.5 * square - 2.0 * frac,
                        -1.5 * square + frac + 0.5, 0.5 * square])
    return weights, slopes


def green_factors(index, length):
    signed = jnp.where(2 * index < length, index, index - length).astype(jnp.float32)
    bspline = 36.0 / (4.0 + 2.0 * jnp.cos(index.astype(jnp.float32) * (2.0 * jnp.pi / length))) ** 2
    bspline = jnp.where(2 * index == length, 0.0, bspline)
    return signed * signed, bspline


def reference(charges, fractions, base_cells, counts):
    slot_index = jnp.arange(charges.shape[0], dtype=jnp.int32)
    live = (slot_index % CAP) < counts.reshape(-1)[slot_index // CAP]
    charge = jnp.where(live, charges, jnp.zeros_like(charges))
    weights_x, slopes_x = spline_weights(fractions[0])
    weights_y, slopes_y = spline_weights(fractions[1])
    weights_z, slopes_z = spline_weights(fractions[2])
    charge_grid = jnp.zeros((GRID, GRID, GRID), jnp.float32)
    for first in range(ORDER):
        for second in range(ORDER):
            for third in range(ORDER):
                cell_x = (base_cells[0] + first) % GRID
                cell_y = (base_cells[1] + second) % GRID
                cell_z = (base_cells[2] + third) % GRID
                charge_grid = charge_grid.at[cell_x, cell_y, cell_z].add(
                    charge * weights_x[first] * weights_y[second] * weights_z[third])
    index = jnp.arange(GRID, dtype=jnp.int32)
    square_line, spline_line = green_factors(index, GRID)
    square = square_line[:, None, None] + square_line[None, :, None] + square_line[None, None, :]
    factor = spline_line[:, None, None] * spline_line[None, :, None] * spline_line[None, None, :]
    green = jnp.where(square > 0.0,
                      coulomb * jnp.exp(square * (-(jnp.pi ** 2) / (ewald * ewald * GRID * GRID))) * factor
                      / (jnp.pi * GRID * jnp.maximum(square, 1.0)), 0.0)
    spectrum = jnp.fft.fftn(charge_grid)
    potential = jnp.real(jnp.fft.ifftn(spectrum * green)) * (GRID ** 3)
    force_x = jnp.zeros_like(charge)
    force_y = jnp.zeros_like(charge)
    force_z = jnp.zeros_like(charge)
    for first in range(ORDER):
        for second in range(ORDER):
            for third in range(ORDER):
                cell_x = (base_cells[0] + first) % GRID
                cell_y = (base_cells[1] + second) % GRID
                cell_z = (base_cells[2] + third) % GRID
                value = potential[cell_x, cell_y, cell_z]
                force_x = force_x + slopes_x[first] * weights_y[second] * weights_z[third] * value
                force_y = force_y + weights_x[first] * slopes_y[second] * weights_z[third] * value
                force_z = force_z + weights_x[first] * weights_y[second] * slopes_z[third] * value
    return -charge[None, :] * jnp.stack([force_x, force_y, force_z])
```

```python
import functools

import jax
import jax.numpy as jnp
import numpy as np
from jax import lax
from jax.experimental import pallas as pl
from jax.experimental.pallas import tpu as pltpu
from jax.sharding import PartitionSpec as P

GRID = 256
ORDER = 4


coulomb = 332.0636
ewald = 0.7
highest = lax.Precision.HIGH
gather_rows = 4


def from_behind(value, axis, steps):
    count = lax.axis_size(axis)
    pairs = [(source, (source + steps) % count) for source in range(count)]
    return lax.ppermute(value, axis, pairs)


def spline_weights(frac):
    rest = 1.0 - frac
    square = frac * frac
    cube = square * frac
    weights = jnp.stack(
        [
            rest * rest * rest / 6.0,
            (3.0 * cube - 6.0 * square + 4.0) / 6.0,
            (-3.0 * cube + 3.0 * square + 3.0 * frac + 1.0) / 6.0,
            cube / 6.0,
        ]
    )
    slopes = jnp.stack(
        [-0.5 * rest * rest, 1.5 * square - 2.0 * frac, -1.5 * square + frac + 0.5, 0.5 * square]
    )
    return (weights, slopes)


def green_factors(index, length):
    signed = jnp.where(2 * index < length, index, index - length).astype(jnp.float32)
    bspline = 36.0 / (4.0 + 2.0 * jnp.cos(index.astype(jnp.float32) * (2.0 * jnp.pi / length))) ** 2
    bspline = jnp.where(2 * index == length, 0.0, bspline)
    return (signed * signed, bspline)


def place_rows(values, lowest, length):
    offset = jnp.arange(length, dtype=jnp.int32)[:, None] - lowest[None, :]
    placed = jnp.zeros((length, lowest.shape[0]), jnp.float32)
    for order_index in range(values.shape[0]):
        placed = placed + jnp.where(offset == order_index, values[order_index][None, :], 0.0)
    return placed


def halves(value):
    high = value.astype(jnp.bfloat16)
    low = (value - high.astype(jnp.float32)).astype(jnp.bfloat16)
    return (high, low)


def rounded_halves(value):
    high = lax.reduce_precision(value, exponent_bits=8, mantissa_bits=7)
    return (high.astype(jnp.bfloat16), (value - high).astype(jnp.bfloat16))


def round_up(value, unit):
    return -(-value // unit) * unit


def spread_kernel(x_ref, y_ref, high_ref, low_ref, out_ref):
    contract = (((1,), (1,)), ((), ()))
    high, low = halves(x_ref[0] * y_ref[...])
    rows = high.shape[0]
    both = jnp.concatenate([high, low], axis=0)
    product = lax.dot_general(both, high_ref[...], contract, preferred_element_type=jnp.float32)
    rest = lax.dot_general(high, low_ref[...], contract, preferred_element_type=jnp.float32)
    out_ref[0] = product[:rows] + (product[rows:] + rest)


def spread(rows_x, rows_y, weighted_z):
    span_x, capacity = rows_x.shape
    pad_y = rows_y.shape[0]
    span_z = weighted_z.shape[0]
    high, low = rounded_halves(weighted_z)
    return pl.pallas_call(
        spread_kernel,
        grid=(span_x,),
        in_specs=[
            pl.BlockSpec((1, 1, capacity), lambda i: (i, 0, 0)),
            pl.BlockSpec((pad_y, capacity), lambda i: (0, 0)),
            pl.BlockSpec((span_z, capacity), lambda i: (0, 0)),
            pl.BlockSpec((span_z, capacity), lambda i: (0, 0)),
        ],
        out_specs=pl.BlockSpec((1, pad_y, span_z), lambda i: (i, 0, 0)),
        out_shape=jax.ShapeDtypeStruct((span_x, pad_y, span_z), jnp.float32),
    )(rows_x[:, None, :], rows_y, high, low)


def gather_kernel(width, pot_ref, z_ref, gz_ref, y_ref, gy_ref, x_ref, gx_ref, out_ref):
    block, pad_y, depth = pot_ref.shape
    capacity = out_ref.shape[1]

    @pl.when(pl.program_id(0) == 0)
    def _():
        out_ref[...] = jnp.zeros_like(out_ref)

    pot = pot_ref[...].reshape(block * pad_y, depth)

    def chunk(c, carry):
        here = pl.ds(pl.multiple_of(c * width, width), width)
        plain = jnp.dot(pot, z_ref[:, here], preferred_element_type=jnp.float32)
        sloped = jnp.dot(pot, gz_ref[:, here], preferred_element_type=jnp.float32)
        weight = y_ref[:, here]
        slope = gy_ref[:, here]
        force_x = out_ref[0:1, here]
        force_y = out_ref[1:2, here]
        force_z = out_ref[2:3, here]
        for i in range(block):
            rows = slice(i * pad_y, (i + 1) * pad_y)
            part = plain[rows]
            row_x = x_ref[i, :, here]
            force_x += gx_ref[i, :, here] * jnp.sum(weight * part, axis=0, keepdims=True)
            force_y += row_x * jnp.sum(slope * part, axis=0, keepdims=True)
            force_z += row_x * jnp.sum(weight * sloped[rows], axis=0, keepdims=True)
        out_ref[0:1, here] = force_x
        out_ref[1:2, here] = force_y
        out_ref[2:3, here] = force_z
        return carry

    lax.fori_loop(0, capacity // width, chunk, 0)


def gather(potential, rows_x, grads_x, rows_y, grads_y, rows_z, grads_z):
    span_x, span_y, span_z = potential.shape
    capacity = rows_x.shape[1]
    pad_y = rows_y.shape[0]
    pad_x = rows_x.shape[0]
    high, low = rounded_halves(potential)
    stacked = jnp.concatenate([high, low, high], axis=2)
    stacked = jnp.pad(stacked, ((0, pad_x - span_x), (0, pad_y - span_y), (0, 0)))
    high, low = rounded_halves(rows_z)
    table = jnp.concatenate([high, high, low], axis=0)
    high, low = rounded_halves(grads_z)
    slope_table = jnp.concatenate([high, high, low], axis=0)
    depth = 3 * span_z

    def whole(rows):
        return pl.BlockSpec((rows, capacity), lambda i: (0, 0))

    line = pl.BlockSpec((gather_rows, 1, capacity), lambda i: (i, 0, 0))
    return pl.pallas_call(
        functools.partial(gather_kernel, 256),
        grid=(pad_x // gather_rows,),
        in_specs=[
            pl.BlockSpec((gather_rows, pad_y, depth), lambda i: (i, 0, 0)),
            whole(depth),
            whole(depth),
            whole(pad_y),
            whole(pad_y),
            line,
            line,
        ],
        out_specs=pl.BlockSpec((3, capacity), lambda i: (0, 0)),
        out_shape=jax.ShapeDtypeStruct((3, capacity), jnp.float32),
    )(stacked, table, slope_table, rows_y, grads_y, rows_x[:, None, :], grads_x[:, None, :])


def y_shift(data, by):
    return from_behind(data, "gy", by)


def z_shift(data, by):
    return from_behind(data, "gz", by)


def exchange(data, axes):
    return lax.all_to_all(data, axes, split_axis=0, concat_axis=0, tiled=True)


def complex_turn(outputs, inputs, sign):
    angle = outputs[:, None] * inputs[None, :] % GRID * (2.0 * np.pi / GRID)
    cosine, sine = np.cos(angle), sign * np.sin(angle)
    return np.array([[cosine, -sine], [sine, cosine]])


def turn(table, data):
    return jnp.dot(
        jnp.asarray(table, jnp.float32),
        data,
        precision=highest,
        preferred_element_type=jnp.float32,
    )


def per_device(charges, fractions, base_cells, counts):

    def x_shift(data, by):
        return from_behind(data, "gx", by)

    count_x = lax.axis_size("gx")
    count_y = lax.axis_size("gy")
    count_z = lax.axis_size("gz")
    index_x = lax.axis_index("gx")
    index_y = lax.axis_index("gy")
    index_z = lax.axis_index("gz")
    cells_x = GRID // count_x
    cells_y = GRID // count_y
    cells_z = GRID // count_z
    ghost_width = ORDER - 1
    span_x = cells_x + ghost_width
    span_y = cells_y + ghost_width
    span_z = cells_z + ghost_width
    planes = count_x * count_y
    width_b = cells_x // count_y
    kept = GRID // 2
    width_k = kept // planes
    width_u = GRID // count_z
    capacity = charges.shape[0]
    live = jnp.arange(capacity, dtype=jnp.int32) < counts.reshape(())
    charge = jnp.where(live, charges, jnp.zeros_like(charges))
    weights_x, slopes_x = spline_weights(fractions[0])
    weights_y, slopes_y = spline_weights(fractions[1])
    weights_z, slopes_z = spline_weights(fractions[2])
    lowest_x = base_cells[0] - index_x * cells_x
    lowest_y = base_cells[1] - index_y * cells_y
    lowest_z = base_cells[2] - index_z * cells_z
    pad_x = round_up(span_x, gather_rows)
    pad_y = round_up(span_y, 16)
    rows_x = place_rows(weights_x, lowest_x, pad_x)
    grads_x = place_rows(slopes_x, lowest_x, pad_x)
    rows_y = place_rows(weights_y, lowest_y, pad_y)
    grads_y = place_rows(slopes_y, lowest_y, pad_y)
    rows_z = place_rows(weights_z, lowest_z, span_z)
    grads_z = place_rows(slopes_z, lowest_z, span_z)
    grid = spread(rows_x[:span_x], rows_y, rows_z * charge[None, :])[:, :span_y]
    arrived = z_shift(grid[:, :, cells_z:], 1)
    grid = jnp.concatenate(
        [grid[:, :, :ghost_width] + arrived, grid[:, :, ghost_width:cells_z]], axis=2
    )
    arrived = x_shift(grid[cells_x:], 1)
    grid = jnp.concatenate([grid[:ghost_width] + arrived, grid[ghost_width:cells_x]], axis=0)
    arrived = y_shift(grid[:, cells_y:], 1)
    grid = jnp.concatenate([grid[:, :ghost_width] + arrived, grid[:, ghost_width:cells_y]], axis=1)
    cell_index = jnp.arange(GRID, dtype=jnp.int32)
    cells = np.arange(GRID)

    data = exchange(grid.reshape(count_y, width_b, cells_y, cells_z), "gy")
    data = data.transpose(0, 2, 1, 3).reshape(GRID, width_b * cells_z)
    table = complex_turn(np.arange(kept), cells, -1.0)[:, 0]
    table = table.reshape(2, planes, width_k, GRID).transpose(1, 0, 2, 3)
    data = turn(table.reshape(2 * kept, GRID), data)
    data = exchange(data.reshape(planes, 2 * width_k, width_b * cells_z), ("gx", "gy"))
    data = data.reshape(planes, 2, width_k, width_b, cells_z).transpose(0, 1, 3, 2, 4)
    table = complex_turn(cells, cells, -1.0).reshape(2, 2, count_z, width_u, planes, width_b)
    table = table.transpose(2, 0, 3, 4, 1, 5).reshape(2 * GRID, 2 * GRID)
    data = turn(table, data.reshape(2 * GRID, width_k * cells_z))
    data = exchange(data.reshape(count_z, 2 * width_u, width_k * cells_z), "gz")
    data = data.reshape(count_z, 2, width_u, width_k, cells_z).transpose(0, 1, 4, 3, 2)
    table = complex_turn(cells, cells, -1.0).reshape(2, 2, GRID, count_z, cells_z)
    table = table.transpose(0, 2, 3, 1, 4).reshape(2 * GRID, 2 * GRID)
    data = turn(table, data.reshape(2 * GRID, width_k * width_u))
    data = data.reshape(2, GRID, width_k * width_u)
    index_ky = (index_x * count_y + index_y) * width_k + jnp.arange(width_k, dtype=jnp.int32)
    index_kx = index_z * width_u + jnp.arange(width_u, dtype=jnp.int32)
    square_y, spline_y = green_factors(index_ky, GRID)
    square_x, spline_x = green_factors(index_kx, GRID)
    square_z, spline_z = green_factors(cell_index, GRID)
    square_yx = (square_y[:, None] + square_x[None, :]).reshape(-1)
    factor_yx = (spline_y[:, None] * spline_x[None, :]).reshape(-1)
    square = square_z[:, None] + square_yx[None, :]
    factor = spline_z[:, None] * factor_yx[None, :]
    green = jnp.where(
        square > 0.0,
        coulomb
        * jnp.exp(square * (-jnp.pi**2 / (ewald * ewald * GRID * GRID)))
        * factor
        / (jnp.pi * GRID * jnp.maximum(square, 1.0)),
        0.0,
    )
    data = data * green[None]
    table = complex_turn(cells, cells, 1.0).reshape(2, 2, count_z, cells_z, GRID)
    table = table.transpose(2, 0, 3, 1, 4).reshape(2 * GRID, 2 * GRID)
    data = turn(table, data.reshape(2 * GRID, width_k * width_u))
    data = exchange(data.reshape(count_z, 2 * cells_z, width_k * width_u), "gz")
    data = data.reshape(count_z, 2, cells_z, width_k, width_u).transpose(0, 1, 4, 3, 2)
    table = complex_turn(cells, cells, 1.0).reshape(2, 2, planes, width_b, count_z, width_u)
    table = table.transpose(2, 0, 3, 4, 1, 5).reshape(2 * GRID, 2 * GRID)
    data = turn(table, data.reshape(2 * GRID, width_k * cells_z))
    data = exchange(data.reshape(planes, 2 * width_b, width_k * cells_z), ("gx", "gy"))
    data = data.reshape(planes, 2, width_b, width_k, cells_z).transpose(0, 1, 3, 2, 4)
    table = complex_turn(cells, np.arange(kept), 1.0)[0]
    table = table * np.where(np.arange(kept) > 0, 2.0, 1.0)
    table = table.reshape(2, GRID, planes, width_k).transpose(1, 2, 0, 3)
    data = turn(table.reshape(GRID, 2 * kept), data.reshape(2 * kept, width_b * cells_z))
    data = exchange(data.reshape(count_y, cells_y, width_b * cells_z), "gy")
    potential = data.reshape(count_y, cells_y, width_b, cells_z).transpose(0, 2, 1, 3)
    potential = potential.reshape(cells_x, cells_y, cells_z)
    arrived = x_shift(potential[:ghost_width], -1)
    potential = jnp.concatenate([potential, arrived], axis=0)
    arrived = y_shift(potential[:, :ghost_width], -1)
    potential = jnp.concatenate([potential, arrived], axis=1)
    arrived = z_shift(potential[:, :, :ghost_width], -1)
    potential = jnp.concatenate([potential, arrived], axis=2)
    return -charge[None, :] * gather(
        potential, rows_x, grads_x, rows_y, grads_y, rows_z, grads_z
    )


def solution(mesh):
    in_specs = (
        P(("gz", "gy", "gx")),
        P(None, ("gz", "gy", "gx")),
        P(None, ("gz", "gy", "gx")),
        P("gz", "gy", "gx"),
    )
    out_specs = P(None, ("gz", "gy", "gx"))
    return jax.shard_map(
        per_device, mesh=mesh, in_specs=in_specs, out_specs=out_specs, check_vma=False
    )
```

```python
import functools

import jax
import jax.numpy as jnp
import numpy as np
from jax import lax
from jax.experimental import pallas as pl
from jax.experimental.pallas import tpu as pltpu
from jax.sharding import PartitionSpec as P

GRID = 256
ORDER = 4


coulomb = 332.0636
ewald = 0.7
highest = lax.Precision.HIGH
gather_rows = 4


def from_behind(value, axis, steps):
    count = lax.axis_size(axis)
    pairs = [(source, (source + steps) % count) for source in range(count)]
    return lax.ppermute(value, axis, pairs)


def spline_weights(frac):
    rest = 1.0 - frac
    square = frac * frac
    cube = square * frac
    weights = jnp.stack(
        [
            rest * rest * rest / 6.0,
            (3.0 * cube - 6.0 * square + 4.0) / 6.0,
            (-3.0 * cube + 3.0 * square + 3.0 * frac + 1.0) / 6.0,
            cube / 6.0,
        ]
    )
    slopes = jnp.stack(
        [-0.5 * rest * rest, 1.5 * square - 2.0 * frac, -1.5 * square + frac + 0.5, 0.5 * square]
    )
    return (weights, slopes)


def green_factors(index, length):
    signed = jnp.where(2 * index < length, index, index - length).astype(jnp.float32)
    bspline = 36.0 / (4.0 + 2.0 * jnp.cos(index.astype(jnp.float32) * (2.0 * jnp.pi / length))) ** 2
    bspline = jnp.where(2 * index == length, 0.0, bspline)
    return (signed * signed, bspline)


def place_rows(values, lowest, length):
    offset = jnp.arange(length, dtype=jnp.int32)[:, None] - lowest[None, :]
    placed = jnp.zeros((length, lowest.shape[0]), jnp.float32)
    for order_index in range(values.shape[0]):
        placed = placed + jnp.where(offset == order_index, values[order_index][None, :], 0.0)
    return placed


def halves(value):
    high = value.astype(jnp.bfloat16)
    low = (value - high.astype(jnp.float32)).astype(jnp.bfloat16)
    return (high, low)


def rounded_halves(value):
    high = lax.reduce_precision(value, exponent_bits=8, mantissa_bits=7)
    return (high.astype(jnp.bfloat16), (value - high).astype(jnp.bfloat16))


def round_up(value, unit):
    return -(-value // unit) * unit


def spread_kernel(x_ref, y_ref, high_ref, low_ref, out_ref):
    contract = (((1,), (1,)), ((), ()))
    block, pad_y, span_z = out_ref.shape
    lines = y_ref[...]
    pairs = jnp.concatenate([x_ref[i] * lines for i in range(block)], axis=0)
    high, low = halves(pairs)
    rows = high.shape[0]
    both = jnp.concatenate([high, low], axis=0)
    product = lax.dot_general(both, high_ref[...], contract, preferred_element_type=jnp.float32)
    rest = lax.dot_general(high, low_ref[...], contract, preferred_element_type=jnp.float32)
    total = product[:rows] + (product[rows:] + rest)
    out_ref[...] = total.reshape(block, pad_y, span_z)


def spread(rows_x, rows_y, weighted_z):
    span_x, capacity = rows_x.shape
    pad_y = rows_y.shape[0]
    span_z = weighted_z.shape[0]
    high, low = rounded_halves(weighted_z)
    return pl.pallas_call(
        spread_kernel,
        grid=(span_x // gather_rows,),
        in_specs=[
            pl.BlockSpec((gather_rows, 1, capacity), lambda i: (i, 0, 0)),
            pl.BlockSpec((pad_y, capacity), lambda i: (0, 0)),
            pl.BlockSpec((span_z, capacity), lambda i: (0, 0)),
            pl.BlockSpec((span_z, capacity), lambda i: (0, 0)),
        ],
        out_specs=pl.BlockSpec((gather_rows, pad_y, span_z), lambda i: (i, 0, 0)),
        out_shape=jax.ShapeDtypeStruct((span_x, pad_y, span_z), jnp.float32),
    )(rows_x[:, None, :], rows_y, high, low)


def gather_kernel(width, pot_ref, z_ref, gz_ref, y_ref, gy_ref, x_ref, gx_ref, out_ref):
    block, pad_y, depth = pot_ref.shape
    capacity = out_ref.shape[1]

    @pl.when(pl.program_id(0) == 0)
    def _():
        out_ref[...] = jnp.zeros_like(out_ref)

    pot = pot_ref[...].reshape(block * pad_y, depth)

    def chunk(c, carry):
        here = pl.ds(pl.multiple_of(c * width, width), width)
        plain = jnp.dot(pot, z_ref[:, here], preferred_element_type=jnp.float32)
        sloped = jnp.dot(pot, gz_ref[:, here], preferred_element_type=jnp.float32)
        weight = y_ref[:, here]
        slope = gy_ref[:, here]
        force_x = out_ref[0:1, here]
        force_y = out_ref[1:2, here]
        force_z = out_ref[2:3, here]
        for i in range(block):
            rows = slice(i * pad_y, (i + 1) * pad_y)
            part = plain[rows]
            row_x = x_ref[i, :, here]
            force_x += gx_ref[i, :, here] * jnp.sum(weight * part, axis=0, keepdims=True)
            force_y += row_x * jnp.sum(slope * part, axis=0, keepdims=True)
            force_z += row_x * jnp.sum(weight * sloped[rows], axis=0, keepdims=True)
        out_ref[0:1, here] = force_x
        out_ref[1:2, here] = force_y
        out_ref[2:3, here] = force_z
        return carry

    lax.fori_loop(0, capacity // width, chunk, 0)


def gather(potential, rows_x, grads_x, rows_y, grads_y, rows_z, grads_z):
    span_x, span_y, span_z = potential.shape
    capacity = rows_x.shape[1]
    pad_y = rows_y.shape[0]
    pad_x = rows_x.shape[0]
    high, low = rounded_halves(potential)
    stacked = jnp.concatenate([high, low, high], axis=2)
    stacked = jnp.pad(stacked, ((0, pad_x - span_x), (0, pad_y - span_y), (0, 0)))
    high, low = rounded_halves(rows_z)
    table = jnp.concatenate([high, high, low], axis=0)
    high, low = rounded_halves(grads_z)
    slope_table = jnp.concatenate([high, high, low], axis=0)
    depth = 3 * span_z

    def whole(rows):
        return pl.BlockSpec((rows, capacity), lambda i: (0, 0))

    line = pl.BlockSpec((gather_rows, 1, capacity), lambda i: (i, 0, 0))
    return pl.pallas_call(
        functools.partial(gather_kernel, 256),
        grid=(pad_x // gather_rows,),
        in_specs=[
            pl.BlockSpec((gather_rows, pad_y, depth), lambda i: (i, 0, 0)),
            whole(depth),
            whole(depth),
            whole(pad_y),
            whole(pad_y),
            line,
            line,
        ],
        out_specs=pl.BlockSpec((3, capacity), lambda i: (0, 0)),
        out_shape=jax.ShapeDtypeStruct((3, capacity), jnp.float32),
    )(stacked, table, slope_table, rows_y, grads_y, rows_x[:, None, :], grads_x[:, None, :])


def y_shift(data, by):
    return from_behind(data, "gy", by)


def z_shift(data, by):
    return from_behind(data, "gz", by)


def exchange(data, axes):
    return lax.all_to_all(data, axes, split_axis=0, concat_axis=0, tiled=True)


def complex_turn(outputs, inputs, sign):
    angle = outputs[:, None] * inputs[None, :] % GRID * (2.0 * np.pi / GRID)
    cosine, sine = np.cos(angle), sign * np.sin(angle)
    return np.array([[cosine, -sine], [sine, cosine]])


def turn(table, data):
    return jnp.dot(
        jnp.asarray(table, jnp.float32),
        data,
        precision=highest,
        preferred_element_type=jnp.float32,
    )


def per_device(charges, fractions, base_cells, counts):

    def x_shift(data, by):
        return from_behind(data, "gx", by)

    count_x = lax.axis_size("gx")
    count_y = lax.axis_size("gy")
    count_z = lax.axis_size("gz")
    index_x = lax.axis_index("gx")
    index_y = lax.axis_index("gy")
    index_z = lax.axis_index("gz")
    cells_x = GRID // count_x
    cells_y = GRID // count_y
    cells_z = GRID // count_z
    ghost_width = ORDER - 1
    span_x = cells_x + ghost_width
    span_y = cells_y + ghost_width
    span_z = cells_z + ghost_width
    planes = count_x * count_y
    width_b = cells_x // count_y
    kept = GRID // 2
    width_k = kept // planes
    width_u = GRID // count_z
    capacity = charges.shape[0]
    live = jnp.arange(capacity, dtype=jnp.int32) < counts.reshape(())
    charge = jnp.where(live, charges, jnp.zeros_like(charges))
    weights_x, slopes_x = spline_weights(fractions[0])
    weights_y, slopes_y = spline_weights(fractions[1])
    weights_z, slopes_z = spline_weights(fractions[2])
    lowest_x = base_cells[0] - index_x * cells_x
    lowest_y = base_cells[1] - index_y * cells_y
    lowest_z = base_cells[2] - index_z * cells_z
    pad_x = round_up(span_x, gather_rows)
    pad_y = round_up(span_y, 16)
    rows_x = place_rows(weights_x, lowest_x, pad_x)
    grads_x = place_rows(slopes_x, lowest_x, pad_x)
    rows_y = place_rows(weights_y, lowest_y, pad_y)
    grads_y = place_rows(slopes_y, lowest_y, pad_y)
    rows_z = place_rows(weights_z, lowest_z, span_z)
    grads_z = place_rows(slopes_z, lowest_z, span_z)
    grid = spread(rows_x, rows_y, rows_z * charge[None, :])[:span_x, :span_y]
    arrived = z_shift(grid[:, :, cells_z:], 1)
    grid = jnp.concatenate(
        [grid[:, :, :ghost_width] + arrived, grid[:, :, ghost_width:cells_z]], axis=2
    )
    arrived = x_shift(grid[cells_x:], 1)
    grid = jnp.concatenate([grid[:ghost_width] + arrived, grid[ghost_width:cells_x]], axis=0)
    arrived = y_shift(grid[:, cells_y:], 1)
    grid = jnp.concatenate([grid[:, :ghost_width] + arrived, grid[:, ghost_width:cells_y]], axis=1)
    cell_index = jnp.arange(GRID, dtype=jnp.int32)
    cells = np.arange(GRID)

    data = exchange(grid.reshape(count_y, width_b, cells_y, cells_z), "gy")
    data = data.transpose(0, 2, 1, 3).reshape(GRID, width_b * cells_z)
    table = complex_turn(np.arange(kept), cells, -1.0)[:, 0]
    table = table.reshape(2, planes, width_k, GRID).transpose(1, 0, 2, 3)
    data = turn(table.reshape(2 * kept, GRID), data)
    data = exchange(data.reshape(planes, 2 * width_k, width_b * cells_z), ("gx", "gy"))
    data = data.reshape(planes, 2, width_k, width_b, cells_z).transpose(0, 1, 3, 2, 4)
    table = complex_turn(cells, cells, -1.0).reshape(2, 2, count_z, width_u, planes, width_b)
    table = table.transpose(2, 0, 3, 4, 1, 5).reshape(2 * GRID, 2 * GRID)
    data = turn(table, data.reshape(2 * GRID, width_k * cells_z))
    data = exchange(data.reshape(count_z, 2 * width_u, width_k * cells_z), "gz")
    data = data.reshape(count_z, 2, width_u, width_k, cells_z).transpose(0, 1, 4, 3, 2)
    table = complex_turn(cells, cells, -1.0).reshape(2, 2, GRID, count_z, cells_z)
    table = table.transpose(0, 2, 3, 1, 4).reshape(2 * GRID, 2 * GRID)
    data = turn(table, data.reshape(2 * GRID, width_k * width_u))
    data = data.reshape(2, GRID, width_k * width_u)
    index_ky = (index_x * count_y + index_y) * width_k + jnp.arange(width_k, dtype=jnp.int32)
    index_kx = index_z * width_u + jnp.arange(width_u, dtype=jnp.int32)
    square_y, spline_y = green_factors(index_ky, GRID)
    square_x, spline_x = green_factors(index_kx, GRID)
    square_z, spline_z = green_factors(cell_index, GRID)
    square_yx = (square_y[:, None] + square_x[None, :]).reshape(-1)
    factor_yx = (spline_y[:, None] * spline_x[None, :]).reshape(-1)
    square = square_z[:, None] + square_yx[None, :]
    factor = spline_z[:, None] * factor_yx[None, :]
    green = jnp.where(
        square > 0.0,
        coulomb
        * jnp.exp(square * (-jnp.pi**2 / (ewald * ewald * GRID * GRID)))
        * factor
        / (jnp.pi * GRID * jnp.maximum(square, 1.0)),
        0.0,
    )
    data = data * green[None]
    table = complex_turn(cells, cells, 1.0).reshape(2, 2, count_z, cells_z, GRID)
    table = table.transpose(2, 0, 3, 1, 4).reshape(2 * GRID, 2 * GRID)
    data = turn(table, data.reshape(2 * GRID, width_k * width_u))
    data = exchange(data.reshape(count_z, 2 * cells_z, width_k * width_u), "gz")
    data = data.reshape(count_z, 2, cells_z, width_k, width_u).transpose(0, 1, 4, 3, 2)
    table = complex_turn(cells, cells, 1.0).reshape(2, 2, planes, width_b, count_z, width_u)
    table = table.transpose(2, 0, 3, 4, 1, 5).reshape(2 * GRID, 2 * GRID)
    data = turn(table, data.reshape(2 * GRID, width_k * cells_z))
    data = exchange(data.reshape(planes, 2 * width_b, width_k * cells_z), ("gx", "gy"))
    data = data.reshape(planes, 2, width_b, width_k, cells_z).transpose(0, 1, 3, 2, 4)
    table = complex_turn(cells, np.arange(kept), 1.0)[0]
    table = table * np.where(np.arange(kept) > 0, 2.0, 1.0)
    table = table.reshape(2, GRID, planes, width_k).transpose(1, 2, 0, 3)
    data = turn(table.reshape(GRID, 2 * kept), data.reshape(2 * kept, width_b * cells_z))
    data = exchange(data.reshape(count_y, cells_y, width_b * cells_z), "gy")
    potential = data.reshape(count_y, cells_y, width_b, cells_z).transpose(0, 2, 1, 3)
    potential = potential.reshape(cells_x, cells_y, cells_z)
    arrived = x_shift(potential[:ghost_width], -1)
    potential = jnp.concatenate([potential, arrived], axis=0)
    arrived = y_shift(potential[:, :ghost_width], -1)
    potential = jnp.concatenate([potential, arrived], axis=1)
    arrived = z_shift(potential[:, :, :ghost_width], -1)
    potential = jnp.concatenate([potential, arrived], axis=2)
    return -charge[None, :] * gather(
        potential, rows_x, grads_x, rows_y, grads_y, rows_z, grads_z
    )


def solution(mesh):
    in_specs = (
        P(("gz", "gy", "gx")),
        P(None, ("gz", "gy", "gx")),
        P(None, ("gz", "gy", "gx")),
        P("gz", "gy", "gx"),
    )
    out_specs = P(None, ("gz", "gy", "gx"))
    return jax.shard_map(
        per_device, mesh=mesh, in_specs=in_specs, out_specs=out_specs, check_vma=False
    )
```
